256 devices in a mesh: energy: 4 (over z_lo), orb: 4 (over x), kpt: 16 (over z_hi, y, core).
Axes of the slice: x: 4, y: 4, z: 8 (z_hi: 2, z_lo: 4; z = z_hi * 4 + z_lo), core: 2. Of those that a mesh axis runs over, the one named last changes fastest.
Arguments:
- lesser: bfloat16 [2, 4, 16, 1, 512, 512], P(None, 'energy', 'kpt', None, None, 'orb'), may hold values from -6 to 6
- coupling: bfloat16 [2, 16, 512, 512], P(None, None, None, 'orb'), may hold values from -0.046875 to 0.046875
- transfer_map: int32 [16, 16], replicated, may hold values from 0 to 15, as said below
Outputs:
- sigma: bfloat16 [2, 4, 16, 1, 512, 512], P(None, None, 'kpt', None, 'energy', 'orb')
The draws below stay inside these ranges and needn't reach their ends.
Inputs may be any that keep to these rules, and one draw needn't show every extreme that they name: transfer_map[k, p] is the index of the momentum transfer k - p: each row and each column holds every number of 0 to 15 once.
All inputs are finite; a program needn't handle non-finite values.
Results may differ from the reference program's by a relative error of at most 0.001.
Values may be sent and summed in bfloat16 or wider, within the bound.
A program may use at most 64 MiB of HBM per device.

```python
import jax
import jax.numpy as jnp
from jax import lax

NO = 512
LAYERS = 1
K = 16
ENERGIES = 4


def draw_transfer_map(key, part):
    ranking = jax.random.permutation(jax.random.fold_in(key, 7), K).astype(jnp.int32)
    target_ids = jnp.arange(K, dtype=jnp.int32)
    shifts = (target_ids[:, None] - target_ids[None, :]) % K
    return ranking[shifts]


def shard_levels(stream_key, shape, shards, low, largest):
    def one(position, parts):
        draws = jax.random.uniform(jax.random.fold_in(jax.random.fold_in(stream_key, 6), position), (parts,), jnp.float32, low / len(shards), largest / len(shards))
        return jnp.repeat(jnp.exp(draws), shape[position] // parts).reshape((-1,) + (1,) * (len(shape) - position - 1))

    factor_of = one(*shards[0])
    for cut in shards[1:]:
        factor_of = factor_of * one(*cut)
    return factor_of


def normal_values(rng, shape, spread, bound, split=(), kind=jnp.bfloat16):
    result = jax.random.normal(rng, shape, jnp.float32) * spread
    if len(split) > 0:
        result = shard_levels(rng, shape, split, -0.22, 0.18) * result
    return jnp.clip(result, min=-bound, max=bound).astype(kind)


def setup_inputs(seed: int = 0) -> dict:
    key_of = jax.random.split(jax.random.key(seed), 4)
    return {
        "lesser": normal_values(key_of[0], (2, ENERGIES, K, LAYERS, NO, NO), 1.0, 6.0, ((1, 4), (2, 16), (5, 4))),
        "coupling": normal_values(key_of[1], (2, K, NO, NO), (2 * NO * K) ** -0.5, 0.046875, ((3, 4),)),
        "transfer_map": draw_transfer_map(jax.random.fold_in(key_of[3], 71), 0),
    }


def reference(lesser, coupling, transfer_map):
    real_green = lesser[0].astype(jnp.float32)
    imag_green = lesser[1].astype(jnp.float32)

    def per_target(target):
        selected = jnp.take(coupling, transfer_map[target], axis=1).astype(jnp.float32)
        real_out = jnp.einsum("eplrm,pmj->elrj", real_green, selected[0]) - jnp.einsum("eplrm,pmj->elrj", imag_green, selected[1])
        imag_out = jnp.einsum("eplrm,pmj->elrj", real_green, selected[1]) + jnp.einsum("eplrm,pmj->elrj", imag_green, selected[0])
        return jnp.stack([real_out, imag_out]).astype(jnp.bfloat16)

    stacked = lax.map(per_target, jnp.arange(K, dtype=jnp.int32))
    return jnp.transpose(stacked, (1, 2, 0, 3, 4, 5))
```

```python
import jax
import jax.numpy as jnp
from jax import lax
from jax.experimental import pallas as pl
from jax.experimental.pallas import tpu as pltpu
from jax.sharding import PartitionSpec as P

MESH = pl.DeviceIdType.MESH
CHUNKS = 2
GROUPS = 4
NEAR_FIRST = (0, 1, 3, 2)


def kernel(lesser, coupling, table, out, src, green, u, y, packed, local_sem, u_sem,
           in_send, in_recv, x_send, x_recv, out_send, out_recv):
    slots = green.shape[2]
    rows = green.shape[4]
    per_group = slots // GROUPS
    z = lax.axis_index("energy")
    x = lax.axis_index("orb")
    k = lax.axis_index("kpt")
    z_hi, row, core = k // 8, (k // 2) % 4, k % 2
    right, left, opposite = (x + 1) % 4, (x + 3) % 4, (x + 2) % 4

    fetch = pltpu.make_async_copy(lesser, src, local_sem)
    fetch.start()
    fetch_u = pltpu.make_async_copy(coupling, u, u_sem)
    fetch_u.start()

    barrier = pltpu.get_barrier_semaphore()

    def greet(i, carry):
        pl.semaphore_signal(
            barrier, inc=1, device_id=((z + 1 + i // 16) % 4, x, (k + i) % 16), device_id_type=MESH
        )
        return carry

    for side in (left, right):
        pl.semaphore_signal(barrier, inc=1, device_id=(z, side, k), device_id_type=MESH)
    lax.fori_loop(0, 48, greet, 0)
    fetch.wait()
    pl.semaphore_wait(barrier, 50)

    def in_copy(chunk, core_to, near, z_hi_to):
        step = 2 * core_to + chunk
        tile = (z + 4 - step) % 4
        shift = 1 + 2 * (tile % 2) if step == 2 else 2
        row_to = (row + 4 - near) % 4
        part = z_hi_to * 4 + row_to
        slot = NEAR_FIRST.index(near) * 4 + z_hi * 2 + core
        begin = pl.multiple_of(tile * 128 + part * rows, rows)
        return pltpu.make_async_remote_copy(
            src_ref=src.at[:, pl.ds(begin, rows), :],
            dst_ref=green.at[chunk, x, slot],
            send_sem=in_send.at[chunk, (NEAR_FIRST.index(near) * 2 + z_hi_to) * 2 + core_to],
            recv_sem=in_recv.at[chunk, slot],
            device_id=((tile + shift) % 4, x, z_hi_to * 8 + row_to * 2 + core_to),
            device_id_type=MESH,
        )

    def all_in(act):
        for chunk in range(CHUNKS):
            for near in NEAR_FIRST:
                for z_hi_to in range(2):
                    for core_to in range(2):
                        act(in_copy(chunk, core_to, near, z_hi_to))

    all_in(lambda copy: copy.start())

    def x_copy(chunk, group, owner, to, lane):
        block = green.at[chunk, owner, pl.ds(group * per_group, per_group)]
        return pltpu.make_async_remote_copy(
            src_ref=block,
            dst_ref=block,
            send_sem=x_send.at[chunk, group, lane],
            recv_sem=x_recv.at[chunk, group, lane],
            device_id=(z, to, k),
            device_id_type=MESH,
        )

    def spread(chunk, group):
        for i in range(per_group):
            slot = group * per_group + i
            landed = green.at[chunk, x, slot]
            pltpu.make_async_remote_copy(
                src_ref=landed, dst_ref=landed, send_sem=in_send.at[chunk, slot],
                recv_sem=in_recv.at[chunk, slot], device_id=(z, right, k), device_id_type=MESH,
            ).wait_recv()
        x_copy(chunk, group, x, right, 0).start()
        x_copy(chunk, group, x, left, 1).start()

    def relay(chunk, group):
        x_copy(chunk, group, left, right, 0).wait_recv()
        if group % 2 == 0:
            x_copy(chunk, group, left, right, 2).start()
        x_copy(chunk, group, right, left, 1).wait_recv()
        if group % 2 == 1:
            x_copy(chunk, group, right, left, 2).start()

    def arrive(chunk, group):
        x_copy(chunk, group, opposite, right, 2).wait_recv()

    def product(chunk):
        def at(t, carry):
            lhs = jnp.concatenate(
                [green[chunk, m].reshape(slots * 2 * rows, 128) for m in range(4)], axis=1
            )
            rhs = jnp.concatenate([u[0, t], u[1, t]], axis=1)
            y[t] = jnp.dot(lhs, rhs, preferred_element_type=jnp.float32).reshape(y.shape[1:])
            return carry
        return at

    def combine(chunk):
        step = 2 * core + chunk
        shift = jnp.where(step == 2, 3 - 2 * (z % 2), 2)
        tile = (z + 4 - shift) % 4
        energy = (tile + step) % 4
        part = k // 2

        def out_copy(target):
            return pltpu.make_async_remote_copy(
                src_ref=packed.at[chunk, target],
                dst_ref=out.at[:, energy, pl.ds(pl.multiple_of(part * rows, rows), rows), :],
                send_sem=out_send.at[chunk, target],
                recv_sem=out_recv.at[energy, part],
                device_id=(tile, x, target),
                device_id_type=MESH,
            )

        def at(i, carry):
            target = (k + i) % 16
            real = jnp.zeros((rows, 128), jnp.float32)
            imag = jnp.zeros((rows, 128), jnp.float32)
            for slot in range(slots):
                near = NEAR_FIRST[slot // 4]
                point = (slot // 2) % 2 * 8 + (row + near) % 4 * 2 + slot % 2
                term = y[table[target, point], slot]
                real += term[0, :, :128] - term[1, :, 128:]
                imag += term[0, :, 128:] + term[1, :, :128]
            packed[chunk, target, 0] = real.astype(packed.dtype)
            packed[chunk, target, 1] = imag.astype(packed.dtype)
            out_copy(target).start()
            return carry

        return at, out_copy

    for group in range(GROUPS):
        spread(0, group)
    for group in range(GROUPS):
        relay(0, group)
        spread(1, group)
    for group in range(GROUPS):
        arrive(0, group)
    fetch_u.wait()
    lax.fori_loop(0, 16, product(0), 0)
    for group in range(GROUPS):
        relay(1, group)
    send0, out_copy0 = combine(0)
    lax.fori_loop(0, 16, send0, 0)
    for group in range(GROUPS):
        arrive(1, group)
    lax.fori_loop(0, 16, product(1), 0)
    send1, out_copy1 = combine(1)
    lax.fori_loop(0, 16, send1, 0)

    all_in(lambda copy: copy.wait_send())
    for chunk in range(CHUNKS):
        for group in range(GROUPS):
            for lane in range(3):
                x_copy(chunk, group, x, right, lane).wait_send()

    def settle(target, carry):
        out_copy0(target).wait_send()
        out_copy1(target).wait_send()
        return carry

    lax.fori_loop(0, 16, settle, 0)

    def collect(i, carry):
        energy, part = i // 8, i % 8
        landed = out.at[:, energy, pl.ds(pl.multiple_of(part * rows, rows), rows), :]
        pltpu.make_async_remote_copy(
            src_ref=packed.at[0, 0], dst_ref=landed, send_sem=out_send.at[0, 0],
            recv_sem=out_recv.at[energy, part], device_id=(z, right, k), device_id_type=MESH,
        ).wait_recv()
        return carry

    lax.fori_loop(0, 32, collect, 0)


def per_device(lesser, coupling, table):
    rows = 16
    result = pl.pallas_call(
        kernel,
        out_shape=jax.ShapeDtypeStruct((2, 4, 128, 128), jnp.bfloat16),
        in_specs=[
            pl.BlockSpec(memory_space=pl.ANY),
            pl.BlockSpec(memory_space=pl.ANY),
            pl.BlockSpec(memory_space=pltpu.SMEM),
        ],
        out_specs=pl.BlockSpec(memory_space=pltpu.VMEM),
        scratch_shapes=[
            pltpu.VMEM((2, 512, 128), jnp.bfloat16),
            pltpu.VMEM((CHUNKS, 4, 16, 2, rows, 128), jnp.bfloat16),
            pltpu.VMEM((2, 16, 512, 128), jnp.bfloat16),
            pltpu.VMEM((16, 16, 2, rows, 256), jnp.float32),
            pltpu.VMEM((CHUNKS, 16, 2, rows, 128), jnp.bfloat16),
            pltpu.SemaphoreType.DMA,
            pltpu.SemaphoreType.DMA,
            pltpu.SemaphoreType.DMA((CHUNKS, 16)),
            pltpu.SemaphoreType.DMA((CHUNKS, 16)),
            pltpu.SemaphoreType.DMA((CHUNKS, GROUPS, 3)),
            pltpu.SemaphoreType.DMA((CHUNKS, GROUPS, 3)),
            pltpu.SemaphoreType.DMA((CHUNKS, 16)),
            pltpu.SemaphoreType.DMA((4, 8)),
        ],
        compiler_params=pltpu.CompilerParams(collective_id=0, has_side_effects=True),
        name="convolve",
    )(lesser.reshape(2, 512, 128), coupling, table)
    return result.reshape(2, 4, 1, 1, 128, 128)


def solution(mesh):
    return jax.shard_map(
        per_device,
        mesh=mesh,
        in_specs=(P(None, "energy", "kpt", None, None, "orb"), P(None, None, None, "orb"), P()),
        out_specs=P(None, None, "kpt", None, "energy", "orb"),
        check_vma=False,
    )
```

```python
import contextlib
import itertools

import jax
import jax.numpy as jnp
from jax import lax
from jax.experimental import pallas as pl
from jax.experimental.pallas import tpu as pltpu
from jax.sharding import PartitionSpec as P

MESH = pl.DeviceIdType.MESH
scope = contextlib.nullcontext
CHUNKS = 2
GROUPS = 8
HALVES = 2
NEAR_FIRST = (0, 1, 3, 2)
X_STEPS = (0, 1, 3, 2)
DEAL = ((0, range(16)), (1, range(16)))
ORDER = (
    "S04", "S05", "S06", "A00", "U", "P00", "S07", "S14", "S15", "S16", "S17", "A10", "P10", "A01",
    "P01", "C0", "A11", "P11", "C1",
)


def kernel(lesser, coupling, table_in, out, src, green, u, y, packed, table, src_sem, u_sem, table_sem, own_sem,
           in_send, near_recv, in_recv, x_send, x_recv, out_send, out_recv):
    slots = green.shape[2]
    rows = green.shape[4]
    per_group = slots // GROUPS
    per_half = slots // HALVES
    z = lax.axis_index("energy")
    x = lax.axis_index("orb")
    k = lax.axis_index("kpt")
    z_hi, row, core = k // 8, (k // 2) % 4, k % 2

    fetch = pltpu.make_async_copy(lesser, src, src_sem)
    fetch.start()
    fetch_u = pltpu.make_async_copy(coupling, u, u_sem)
    fetch_u.start()
    own = []
    for chunk in range(CHUNKS):
        begin = pl.multiple_of((z + 4 - 2 * core - chunk) % 4 * 128 + k // 2 * rows, rows)
        own.append(
            pltpu.make_async_copy(
                lesser.at[:, pl.ds(begin, rows), :], green.at[chunk, x, 0], own_sem.at[chunk]
            )
        )
        own[-1].start()
    fetch_table = pltpu.make_async_copy(table_in, table, table_sem)
    fetch_table.start()

    def fetched():
        fetch_u.wait()
        fetch_table.wait()

    barrier = pltpu.get_barrier_semaphore()

    def greet(z_to, x_to, k_to):
        pl.semaphore_signal(barrier, inc=1, device_id=(z_to, x_to, k_to), device_id_type=MESH)

    def greet_near(i, carry):
        other = (x * 8 + k % 8 + i) % 32
        greet(z, other // 8, z_hi * 8 + other % 8)
        return carry

    def greet_far(i, carry):
        greet(z, x, (k + 8) // 8 % 2 * 8 + i)
        greet((z + 1) % 4, x, 2 * i)
        greet((z + 2) % 4, x, 2 * i + 1)
        greet((z + 3) % 4, x, 2 * i + 1)
        return carry

    lax.fori_loop(1, 32, greet_near, 0)
    lax.fori_loop(0, 8, greet_far, 0)
    with scope("s_fetch"):
        fetch.wait()
    with scope("s_barrier"):
        pl.semaphore_wait(barrier, 55 + 16 * core)

    def send(source, target, send_sem, recv_sem, place):
        return pltpu.make_async_remote_copy(
            src_ref=source, dst_ref=target, send_sem=send_sem, recv_sem=recv_sem,
            device_id=place, device_id_type=MESH,
        )

    def landed(block, recv_sem):
        send(block, block, x_send, recv_sem, (z, (x + 1) % 4, k)).wait_recv()

    def sent(block, send_sem):
        send(block, block, send_sem, out_recv, (z, (x + 1) % 4, k)).wait_send()

    places = tuple(itertools.product(range(2), NEAR_FIRST, range(2)))

    def deal(chunk, slot, x_step):
        z_step, near, core_step = places[slot]
        z_hi_to, row_to, core_to = (z_hi + z_step) % 2, (row + 4 - near) % 4, (core + core_step) % 2
        tile = (z + 4 - 2 * core_to - chunk) % 4
        begin = pl.multiple_of(tile * 128 + (z_hi_to * 4 + row_to) * rows, rows)
        send(
            src.at[:, pl.ds(begin, rows), :],
            green.at[chunk, x, slot],
            in_send,
            in_recv.at[chunk, slot // per_group] if z_step else near_recv.at[chunk],
            (z, (x + x_step) % 4, z_hi_to * 8 + row_to * 2 + core_to),
        ).start()

    for chunk, slots_of in DEAL:
        for slot in slots_of:
            for x_step in (0,) if slot >= per_half else X_STEPS:
                if (slot, x_step) != (0, 0):
                    deal(chunk, slot, x_step)

    def spread(chunk, group):
        block = green.at[chunk, x, pl.ds(group * per_group, per_group)]
        landed(block, in_recv.at[chunk, group])
        for x_step in X_STEPS[1:]:
            send(block, block, x_send, x_recv.at[chunk], (z, (x + x_step) % 4, k)).start()

    def arrive(chunk, half):
        if half:
            landed(green.at[chunk, pl.ds(0, 3), pl.ds(0, per_half)], x_recv.at[chunk])
        else:
            own[chunk].wait()
            landed(packed.at[pl.ds(0, 31)], near_recv.at[chunk])

    def product(chunk, half, extra=None):
        part = pl.ds(half * per_half, per_half)

        def at(t, carry):
            lhs = jnp.concatenate(
                [green[chunk, m, part].reshape(per_half * 2 * rows, 128) for m in range(4)], axis=1
            )
            rhs = jnp.concatenate([u[0, t], u[1, t]], axis=1)
            terms = jnp.dot(lhs, rhs, preferred_element_type=jnp.float32)
            y[chunk, t, part] = terms.reshape(per_half, 2, rows, 256)
            if extra is not None:
                total(extra, t)
            return carry

        lax.fori_loop(0, 16, at, 0, unroll=True)

    def target_of(i):
        far = jnp.where(i < 8, 2 + i // 4, 3 - i // 4)
        return (z_hi + 1 + i // 2) % 2 * 8 + (row + far) % 4 * 2 + (core + 1 + i) % 2

    def total(chunk, i):
        target = target_of(i)
        real = jnp.zeros((rows, 128), jnp.float32)
        imag = jnp.zeros((rows, 128), jnp.float32)
        for slot in range(slots):
            z_step, near, core_step = places[slot]
            point = (z_hi + z_step) % 2 * 8 + (row + near) % 4 * 2 + (core + core_step) % 2
            term = y[chunk, table[target, point], slot]
            real += term[0, :, :128] - term[1, :, 128:]
            imag += term[0, :, 128:] + term[1, :, :128]
        packed[chunk * 16 + i, 0] = real.astype(packed.dtype)
        packed[chunk * 16 + i, 1] = imag.astype(packed.dtype)

    def give(chunk, i):
        tile = (z + 4 - 2 * core - chunk) % 4
        begin = pl.ds(pl.multiple_of(k // 2 * rows, rows), rows)

        def away():
            send(
                packed.at[chunk * 16 + i], out.at[:, z, begin, :], out_send, out_recv,
                (tile, x, target_of(i)),
            ).start()

        if chunk > 0:
            away()
        else:
            stays = jnp.logical_and(core == 0, i == 15)
            pl.when(jnp.logical_not(stays))(away)

            @pl.when(stays)
            def _():
                out[:, z, begin, :] = packed[15]

    def combine(chunk):
        def at(i, carry):
            total(chunk, i)
            give(chunk, i)
            return carry

        lax.fori_loop(0, 16, at, 0)

    def give_all(chunk):
        def at(i, carry):
            give(chunk, i)
            return carry

        lax.fori_loop(0, 16, at, 0)

    def product_and_total(chunk, half):
        product(chunk, half, chunk - 1)

    act = {
        "S": spread, "A": arrive, "P": product, "C": combine, "U": fetched, "F": product_and_total, "G": give_all,
    }
    for name in ORDER:
        with scope("s_" + name):
            act[name[0]](*(int(digit) for digit in name[1:]))

    with scope("s_drain"):
        sent(green.at[:, pl.ds(0, 3), pl.ds(0, 13)], in_send)
        sent(green.at[:, pl.ds(0, 3), pl.ds(0, per_half)], x_send)
        for count in (31, 32):

            @pl.when(core == count - 31)
            def _():
                sent(packed.at[pl.ds(0, count)], out_send)
    with scope("s_collect"):
        for count in (31, 32):

            @pl.when(core == count - 31)
            def _():
                landed(packed.at[pl.ds(0, count)], out_recv)


def per_device(lesser, coupling, table):
    rows = 16
    result = pl.pallas_call(
        kernel,
        out_shape=pltpu.VMEM((2, 4, 128, 128), jnp.bfloat16),
        in_specs=[
            pl.BlockSpec(memory_space=pl.ANY),
            pl.BlockSpec(memory_space=pl.ANY),
            pl.BlockSpec(memory_space=pl.ANY),
        ],
        out_specs=pl.BlockSpec(memory_space=pltpu.VMEM),
        scratch_shapes=[
            pltpu.VMEM((2, 512, 128), jnp.bfloat16),
            pltpu.VMEM((CHUNKS, 4, 16, 2, rows, 128), jnp.bfloat16),
            pltpu.VMEM((2, 16, 512, 128), jnp.bfloat16),
            pltpu.VMEM((CHUNKS, 16, 16, 2, rows, 256), jnp.float32),
            pltpu.VMEM((CHUNKS * 16, 2, rows, 128), jnp.bfloat16),
            pltpu.SMEM((16, 16), jnp.int32),
            pltpu.SemaphoreType.DMA,
            pltpu.SemaphoreType.DMA,
            pltpu.SemaphoreType.DMA,
            pltpu.SemaphoreType.DMA((CHUNKS,)),
            pltpu.SemaphoreType.DMA,
            pltpu.SemaphoreType.DMA((CHUNKS,)),
            pltpu.SemaphoreType.DMA((CHUNKS, GROUPS)),
            pltpu.SemaphoreType.DMA,
            pltpu.SemaphoreType.DMA((CHUNKS,)),
            pltpu.SemaphoreType.DMA,
            pltpu.SemaphoreType.DMA,
        ],
        compiler_params=pltpu.CompilerParams(collective_id=0, has_side_effects=True),
        name="convolve",
    )(lesser.reshape(2, 512, 128), coupling, table)
    return result.reshape(2, 4, 1, 1, 128, 128)


def solution(mesh):
    return jax.shard_map(
        per_device,
        mesh=mesh,
        in_specs=(P(None, "energy", "kpt", None, None, "orb"), P(None, None, None, "orb"), P()),
        out_specs=P(None, None, "kpt", None, "energy", "orb"),
        check_vma=False,
    )
```

```python
import contextlib
import itertools

import jax
import jax.numpy as jnp
from jax import lax
from jax.experimental import pallas as pl
from jax.experimental.pallas import tpu as pltpu
from jax.sharding import PartitionSpec as P

MESH = pl.DeviceIdType.MESH
scope = contextlib.nullcontext
CHUNKS = 2
GROUPS = 8
HALVES = 2
NEAR_FIRST = (0, 1, 3, 2)
X_STEPS = (0, 1, 3, 2)
FLIGHT = 1
DEAL = ((0, range(16)), (1, range(16)))
ORDER = (
    "S01", "S02", "S03", "S11", "S12", "S13", "S04", "S05", "S06", "S07", "A00", "U", "P00", "S14",
    "S15", "S16", "S17", "A10", "P10", "A01", "P01", "C0", "A11", "P11", "C1",
)


def kernel(lesser, coupling, table_in, out, src, green, u, y, packed, table, src_sem, u_sem, table_sem, own_sem,
           in_send, near_recv, in_recv, x_send, x_recv, out_send, out_recv):
    slots = green.shape[2]
    rows = green.shape[4]
    per_group = slots // GROUPS
    per_half = slots // HALVES
    z = lax.axis_index("energy")
    x = lax.axis_index("orb")
    k = lax.axis_index("kpt")
    z_hi, row, core = k // 8, (k // 2) % 4, k % 2

    fetch = pltpu.make_async_copy(lesser, src, src_sem)
    fetch.start()
    fetch_u = pltpu.make_async_copy(coupling, u, u_sem)
    fetch_u.start()
    own = []
    for chunk in range(CHUNKS):
        begin = pl.multiple_of((z + 4 - 2 * core - chunk) % 4 * 128 + k // 2 * rows, rows)
        own.append(
            pltpu.make_async_copy(
                lesser.at[:, pl.ds(begin, rows), :], green.at[chunk, x, 0], own_sem.at[chunk]
            )
        )
        own[-1].start()
    fetch_table = pltpu.make_async_copy(table_in, table, table_sem)
    fetch_table.start()

    def fetched():
        fetch_u.wait()
        fetch_table.wait()

    barrier = pltpu.get_barrier_semaphore()

    def greet(z_to, x_to, k_to):
        pl.semaphore_signal(barrier, inc=1, device_id=(z_to, x_to, k_to), device_id_type=MESH)

    def greet_near(i, carry):
        other = (x * 8 + k % 8 + i) % 32
        greet(z, other // 8, z_hi * 8 + other % 8)
        return carry

    def greet_far(i, carry):
        greet(z, x, (k + 8) // 8 % 2 * 8 + i)
        greet((z + 1) % 4, x, 2 * i)
        greet((z + 2) % 4, x, 2 * i + 1)
        greet((z + 3) % 4, x, 2 * i + 1)
        return carry

    lax.fori_loop(0, 8, greet_far, 0, unroll=True)
    lax.fori_loop(1, 32, greet_near, 0, unroll=True)
    with scope("s_fetch"):
        fetch.wait()
    with scope("s_barrier"):
        pl.semaphore_wait(barrier, 55 + 16 * core)

    def send(source, target, send_sem, recv_sem, place):
        return pltpu.make_async_remote_copy(
            src_ref=source, dst_ref=target, send_sem=send_sem, recv_sem=recv_sem,
            device_id=place, device_id_type=MESH,
        )

    def landed(block, recv_sem):
        send(block, block, x_send, recv_sem, (z, (x + 1) % 4, k)).wait_recv()

    def sent(block, send_sem):
        send(block, block, send_sem, out_recv, (z, (x + 1) % 4, k)).wait_send()

    places = tuple(itertools.product(range(2), NEAR_FIRST, range(2)))

    def deal(chunk, slot, x_step):
        z_step, near, core_step = places[slot]
        z_hi_to, row_to, core_to = (z_hi + z_step) % 2, (row + 4 - near) % 4, (core + core_step) % 2
        tile = (z + 4 - 2 * core_to - chunk) % 4
        begin = pl.multiple_of(tile * 128 + (z_hi_to * 4 + row_to) * rows, rows)
        send(
            src.at[:, pl.ds(begin, rows), :],
            green.at[chunk, x, slot],
            in_send,
            near_recv.at[chunk] if slot < FLIGHT * per_group else in_recv.at[chunk, slot // per_group],
            (z, (x + x_step) % 4, z_hi_to * 8 + row_to * 2 + core_to),
        ).start()

    for chunk, slots_of in DEAL:
        for slot in slots_of:
            for x_step in X_STEPS if slot < FLIGHT * per_group else (0,):
                if (slot, x_step) != (0, 0):
                    deal(chunk, slot, x_step)

    def spread(chunk, group):
        block = green.at[chunk, x, pl.ds(group * per_group, per_group)]
        landed(block, in_recv.at[chunk, group])
        for x_step in X_STEPS[1:]:
            send(block, block, x_send, x_recv.at[chunk, group * HALVES // GROUPS], (z, (x + x_step) % 4, k)).start()

    def arrive(chunk, half):
        spreads = GROUPS // HALVES
        if half == 0:
            own[chunk].wait()
            landed(packed.at[pl.ds(0, 4 * per_group * FLIGHT - 1)], near_recv.at[chunk])
            spreads -= FLIGHT
        if spreads:
            landed(packed.at[pl.ds(0, 3 * per_group * spreads)], x_recv.at[chunk, half])

    def product(chunk, half, extra=None):
        part = pl.ds(half * per_half, per_half)

        def at(t, carry):
            lhs = jnp.concatenate(
                [green[chunk, m, part].reshape(per_half * 2 * rows, 128) for m in range(4)], axis=1
            )
            rhs = jnp.concatenate([u[0, t], u[1, t]], axis=1)
            terms = jnp.dot(lhs, rhs, preferred_element_type=jnp.float32)
            y[chunk, t, part] = terms.reshape(per_half, 2, rows, 256)
            if extra is not None:
                total(extra, t)
            return carry

        lax.fori_loop(0, 16, at, 0, unroll=True)

    wraps = z == 3 * core

    def target_of(chunk, i):
        far = jnp.where(i % 8 < 4, 2 + i % 8 // 2, 3 - i % 8 // 2)
        z_step = 1 - i // 8
        if chunk:
            z_step = jnp.where(wraps, i // 8, z_step)
        return (z_hi + z_step) % 2 * 8 + (row + far) % 4 * 2 + (core + 1 + i) % 2

    def total(chunk, i):
        target = target_of(chunk, i)
        real = jnp.zeros((rows, 128), jnp.float32)
        imag = jnp.zeros((rows, 128), jnp.float32)
        for slot in range(slots):
            z_step, near, core_step = places[slot]
            point = (z_hi + z_step) % 2 * 8 + (row + near) % 4 * 2 + (core + core_step) % 2
            term = y[chunk, table[target, point], slot]
            real += term[0, :, :128] - term[1, :, 128:]
            imag += term[0, :, 128:] + term[1, :, :128]
        packed[chunk * 16 + i, 0] = real.astype(packed.dtype)
        packed[chunk * 16 + i, 1] = imag.astype(packed.dtype)

    def give(chunk, i):
        tile = (z + 4 - 2 * core - chunk) % 4
        begin = pl.ds(pl.multiple_of(k // 2 * rows, rows), rows)

        def away():
            send(
                packed.at[chunk * 16 + i], out.at[:, z, begin, :], out_send, out_recv,
                (tile, x, target_of(chunk, i)),
            ).start()

        if chunk > 0:
            away()
        else:
            stays = jnp.logical_and(core == 0, i == 15)
            pl.when(jnp.logical_not(stays))(away)

            @pl.when(stays)
            def _():
                out[:, z, begin, :] = packed[15]

    def combine(chunk):
        def at(i, carry):
            total(chunk, i)
            give(chunk, i)
            return carry

        lax.fori_loop(0, 16, at, 0)

    def give_all(chunk):
        def at(i, carry):
            give(chunk, i)
            return carry

        lax.fori_loop(0, 16, at, 0)

    def product_and_total(chunk, half):
        product(chunk, half, chunk - 1)

    act = {
        "S": spread, "A": arrive, "P": product, "C": combine, "U": fetched, "F": product_and_total, "G": give_all,
    }
    for name in ORDER:
        with scope("s_" + name):
            act[name[0]](*(int(digit) for digit in name[1:]))

    with scope("s_drain"):
        sent(u.at[:, pl.ds(0, 3), pl.ds(0, 160 + 64 * FLIGHT), :], in_send)
        sent(u.at[:, pl.ds(0, 4), pl.ds(0, 384 - 48 * FLIGHT), :], x_send)
        for count in (31, 32):

            @pl.when(core == count - 31)
            def _():
                sent(packed.at[pl.ds(0, count)], out_send)
    with scope("s_collect"):
        for count in (31, 32):

            @pl.when(core == count - 31)
            def _():
                landed(packed.at[pl.ds(0, count)], out_recv)


def per_device(lesser, coupling, table):
    rows = 16
    result = pl.pallas_call(
        kernel,
        out_shape=pltpu.VMEM((2, 4, 128, 128), jnp.bfloat16),
        in_specs=[
            pl.BlockSpec(memory_space=pl.ANY),
            pl.BlockSpec(memory_space=pl.ANY),
            pl.BlockSpec(memory_space=pl.ANY),
        ],
        out_specs=pl.BlockSpec(memory_space=pltpu.VMEM),
        scratch_shapes=[
            pltpu.VMEM((2, 512, 128), jnp.bfloat16),
            pltpu.VMEM((CHUNKS, 4, 16, 2, rows, 128), jnp.bfloat16),
            pltpu.VMEM((2, 16, 512, 128), jnp.bfloat16),
            pltpu.VMEM((CHUNKS, 16, 16, 2, rows, 256), jnp.float32),
            pltpu.VMEM((CHUNKS * 16, 2, rows, 128), jnp.bfloat16),
            pltpu.SMEM((16, 16), jnp.int32),
            pltpu.SemaphoreType.DMA,
            pltpu.SemaphoreType.DMA,
            pltpu.SemaphoreType.DMA,
            pltpu.SemaphoreType.DMA((CHUNKS,)),
            pltpu.SemaphoreType.DMA,
            pltpu.SemaphoreType.DMA((CHUNKS,)),
            pltpu.SemaphoreType.DMA((CHUNKS, GROUPS)),
            pltpu.SemaphoreType.DMA,
            pltpu.SemaphoreType.DMA((CHUNKS, HALVES)),
            pltpu.SemaphoreType.DMA,
            pltpu.SemaphoreType.DMA,
        ],
        compiler_params=pltpu.CompilerParams(collective_id=0, has_side_effects=True),
        name="convolve",
    )(lesser.reshape(2, 512, 128), coupling, table)
    return result.reshape(2, 4, 1, 1, 128, 128)


def solution(mesh):
    return jax.shard_map(
        per_device,
        mesh=mesh,
        in_specs=(P(None, "energy", "kpt", None, None, "orb"), P(None, None, None, "orb"), P()),
        out_specs=P(None, None, "kpt", None, "energy", "orb"),
        check_vma=False,
    )
```

```python
import contextlib
import itertools

import jax
import jax.numpy as jnp
from jax import lax
from jax.experimental import pallas as pl
from jax.experimental.pallas import tpu as pltpu
from jax.sharding import PartitionSpec as P

MESH = pl.DeviceIdType.MESH
scope = contextlib.nullcontext
CHUNKS = 2
GROUPS = 8
HALVES = 2
NEAR_FIRST = (0, 1, 3, 2)
X_STEPS = (0, 1, 3, 2)
FLIGHT = 1
DEAL = ((0, range(16)), (1, range(16)))
ORDER = (
    "S01", "S02", "S03", "S11", "S12", "S04", "S13", "S05", "S06", "S07", "A002", "U", "P002", "S14",
    "S15", "S16", "S17", "A102", "P102", "A023", "P023", "A034", "P034", "C0", "A123", "P123", "A134",
    "P134", "C1",
)


def kernel(lesser, coupling, table_in, out, src, green, u, y, packed, table, src_sem, u_sem, table_sem, own_sem,
           in_send, near_recv, in_recv, x_send, x_recv, out_send, out_recv):
    slots = green.shape[2]
    rows = green.shape[4]
    per_group = slots // GROUPS
    per_half = slots // HALVES
    z = lax.axis_index("energy")
    x = lax.axis_index("orb")
    k = lax.axis_index("kpt")
    z_hi, row, core = k // 8, (k // 2) % 4, k % 2

    fetch = pltpu.make_async_copy(lesser, src, src_sem)
    fetch.start()
    fetch_u = pltpu.make_async_copy(coupling, u, u_sem)
    fetch_u.start()
    own = []
    for chunk in range(CHUNKS):
        begin = pl.multiple_of((z + 4 - 2 * core - chunk) % 4 * 128 + k // 2 * rows, rows)
        own.append(
            pltpu.make_async_copy(
                lesser.at[:, pl.ds(begin, rows), :], green.at[chunk, x, 0], own_sem.at[chunk]
            )
        )
        own[-1].start()
    fetch_table = pltpu.make_async_copy(table_in, table, table_sem)
    fetch_table.start()

    def fetched():
        fetch_u.wait()
        fetch_table.wait()

    barrier = pltpu.get_barrier_semaphore()

    def greet(z_to, x_to, k_to):
        pl.semaphore_signal(barrier, inc=1, device_id=(z_to, x_to, k_to), device_id_type=MESH)

    def greet_near(i, carry):
        other = (x * 8 + k % 8 + i) % 32
        greet(z, other // 8, z_hi * 8 + other % 8)
        return carry

    def greet_far(i, carry):
        greet(z, x, (k + 8) // 8 % 2 * 8 + i)
        greet((z + 1) % 4, x, 2 * i)
        greet((z + 2) % 4, x, 2 * i + 1)
        greet((z + 3) % 4, x, 2 * i + 1)
        return carry

    lax.fori_loop(0, 8, greet_far, 0, unroll=True)
    lax.fori_loop(1, 32, greet_near, 0, unroll=True)
    with scope("s_fetch"):
        fetch.wait()
    with scope("s_barrier"):
        pl.semaphore_wait(barrier, 55 + 16 * core)

    def send(source, target, send_sem, recv_sem, place):
        return pltpu.make_async_remote_copy(
            src_ref=source, dst_ref=target, send_sem=send_sem, recv_sem=recv_sem,
            device_id=place, device_id_type=MESH,
        )

    def landed(block, recv_sem):
        send(block, block, x_send, recv_sem, (z, (x + 1) % 4, k)).wait_recv()

    def sent(block, send_sem):
        send(block, block, send_sem, out_recv, (z, (x + 1) % 4, k)).wait_send()

    places = tuple(itertools.product(range(2), NEAR_FIRST, range(2)))

    def deal(chunk, slot, x_step):
        z_step, near, core_step = places[slot]
        z_hi_to, row_to, core_to = (z_hi + z_step) % 2, (row + 4 - near) % 4, (core + core_step) % 2
        tile = (z + 4 - 2 * core_to - chunk) % 4
        begin = pl.multiple_of(tile * 128 + (z_hi_to * 4 + row_to) * rows, rows)
        send(
            src.at[:, pl.ds(begin, rows), :],
            green.at[chunk, x, slot],
            in_send,
            near_recv.at[chunk] if slot < FLIGHT * per_group else in_recv.at[chunk, slot // per_group],
            (z, (x + x_step) % 4, z_hi_to * 8 + row_to * 2 + core_to),
        ).start()

    for chunk, slots_of in DEAL:
        for slot in slots_of:
            for x_step in X_STEPS if slot < FLIGHT * per_group else (0,):
                if (slot, x_step) != (0, 0):
                    deal(chunk, slot, x_step)

    def spread(chunk, group):
        block = green.at[chunk, x, pl.ds(group * per_group, per_group)]
        landed(block, in_recv.at[chunk, group])
        for x_step in X_STEPS[1:]:
            send(block, block, x_send, x_recv.at[chunk, group * 4 // GROUPS], (z, (x + x_step) % 4, k)).start()

    def arrive(chunk, first, last):
        if first == 0:
            own[chunk].wait()
            landed(packed.at[pl.ds(0, 4 * per_group * FLIGHT - 1)], near_recv.at[chunk])
        for quarter in range(first, last):
            spreads = GROUPS // 4 - (FLIGHT if quarter == 0 else 0)
            landed(packed.at[pl.ds(0, 3 * per_group * spreads)], x_recv.at[chunk, quarter])

    def product(chunk, first, last):
        count = slots // 4 * (last - first)
        part = pl.ds(slots // 4 * first, count)

        def at(t, carry):
            lhs = jnp.concatenate(
                [green[chunk, m, part].reshape(count * 2 * rows, 128) for m in range(4)], axis=1
            )
            rhs = jnp.concatenate([u[0, t], u[1, t]], axis=1)
            terms = jnp.dot(lhs, rhs, preferred_element_type=jnp.float32)
            y[chunk, t, part] = terms.reshape(count, 2, rows, 256)
            return carry

        lax.fori_loop(0, 16, at, 0, unroll=True)

    wraps = z == 3 * core

    def target_of(chunk, i):
        far = jnp.where(i % 8 < 4, 2 + i % 8 // 2, 3 - i % 8 // 2)
        z_step = 1 - i // 8
        if chunk:
            z_step = jnp.where(wraps, i // 8, z_step)
        return (z_hi + z_step) % 2 * 8 + (row + far) % 4 * 2 + (core + 1 + i) % 2

    def total(chunk, i):
        target = target_of(chunk, i)
        real = jnp.zeros((rows, 128), jnp.float32)
        imag = jnp.zeros((rows, 128), jnp.float32)
        for slot in range(slots):
            z_step, near, core_step = places[slot]
            point = (z_hi + z_step) % 2 * 8 + (row + near) % 4 * 2 + (core + core_step) % 2
            term = y[chunk, table[target, point], slot]
            real += term[0, :, :128] - term[1, :, 128:]
            imag += term[0, :, 128:] + term[1, :, :128]
        packed[chunk * 16 + i, 0] = real.astype(packed.dtype)
        packed[chunk * 16 + i, 1] = imag.astype(packed.dtype)

    def give(chunk, i):
        tile = (z + 4 - 2 * core - chunk) % 4
        begin = pl.ds(pl.multiple_of(k // 2 * rows, rows), rows)

        def away():
            send(
                packed.at[chunk * 16 + i], out.at[:, z, begin, :], out_send, out_recv,
                (tile, x, target_of(chunk, i)),
            ).start()

        if chunk > 0:
            away()
        else:
            stays = jnp.logical_and(core == 0, i == 15)
            pl.when(jnp.logical_not(stays))(away)

            @pl.when(stays)
            def _():
                out[:, z, begin, :] = packed[15]

    def combine(chunk):
        def at(i, carry):
            total(chunk, i)
            give(chunk, i)
            return carry

        lax.fori_loop(0, 16, at, 0, unroll=True)

    act = {
        "S": spread, "A": arrive, "P": product, "C": combine, "U": fetched,
    }
    for name in ORDER:
        with scope("s_" + name):
            act[name[0]](*(int(digit) for digit in name[1:]))

    with scope("s_drain"):
        sent(u.at[:, pl.ds(0, 3), pl.ds(0, 160 + 64 * FLIGHT), :], in_send)
        sent(u.at[:, pl.ds(0, 4), pl.ds(0, 384 - 48 * FLIGHT), :], x_send)
        for count in (31, 32):

            @pl.when(core == count - 31)
            def _():
                sent(packed.at[pl.ds(0, count)], out_send)
    with scope("s_collect"):
        for count in (31, 32):

            @pl.when(core == count - 31)
            def _():
                landed(packed.at[pl.ds(0, count)], out_recv)


def per_device(lesser, coupling, table):
    rows = 16
    result = pl.pallas_call(
        kernel,
        out_shape=pltpu.VMEM((2, 4, 128, 128), jnp.bfloat16),
        in_specs=[
            pl.BlockSpec(memory_space=pl.ANY),
            pl.BlockSpec(memory_space=pl.ANY),
            pl.BlockSpec(memory_space=pl.ANY),
        ],
        out_specs=pl.BlockSpec(memory_space=pltpu.VMEM),
        scratch_shapes=[
            pltpu.VMEM((2, 512, 128), jnp.bfloat16),
            pltpu.VMEM((CHUNKS, 4, 16, 2, rows, 128), jnp.bfloat16),
            pltpu.VMEM((2, 16, 512, 128), jnp.bfloat16),
            pltpu.VMEM((CHUNKS, 16, 16, 2, rows, 256), jnp.float32),
            pltpu.VMEM((CHUNKS * 16, 2, rows, 128), jnp.bfloat16),
            pltpu.SMEM((16, 16), jnp.int32),
            pltpu.SemaphoreType.DMA,
            pltpu.SemaphoreType.DMA,
            pltpu.SemaphoreType.DMA,
            pltpu.SemaphoreType.DMA((CHUNKS,)),
            pltpu.SemaphoreType.DMA,
            pltpu.SemaphoreType.DMA((CHUNKS,)),
            pltpu.SemaphoreType.DMA((CHUNKS, GROUPS)),
            pltpu.SemaphoreType.DMA,
            pltpu.SemaphoreType.DMA((CHUNKS, 4)),
            pltpu.SemaphoreType.DMA,
            pltpu.SemaphoreType.DMA,
        ],
        compiler_params=pltpu.CompilerParams(collective_id=0, has_side_effects=True),
        name="convolve",
    )(lesser.reshape(2, 512, 128), coupling, table)
    return result.reshape(2, 4, 1, 1, 128, 128)


def solution(mesh):
    return jax.shard_map(
        per_device,
        mesh=mesh,
        in_specs=(P(None, "energy", "kpt", None, None, "orb"), P(None, None, None, "orb"), P()),
        out_specs=P(None, None, "kpt", None, "energy", "orb"),
        check_vma=False,
    )
```

```python
import contextlib
import itertools

import jax
import jax.numpy as jnp
from jax import lax
from jax.experimental import pallas as pl
from jax.experimental.pallas import tpu as pltpu
from jax.sharding import PartitionSpec as P

MESH = pl.DeviceIdType.MESH
scope = contextlib.nullcontext
CHUNKS = 2
GROUPS = 8
HALVES = 2
NEAR_FIRST = (0, 1, 3, 2)
X_STEPS = (0, 2, 1, 3)
FLIGHT = 1
DEAL = ((0, range(16)), (1, range(16)))
ORDER = (
    "S01", "S02", "S03", "S11", "S12", "S04", "S13", "S05", "S06", "S07", "A002", "U", "P002", "S14",
    "S15", "S16", "S17", "A102", "P102", "A023", "P023", "A034", "P034", "C0", "A123", "P123", "A134",
    "P134", "C1",
)


def kernel(lesser, coupling, table_in, out, src, green, u, y, packed, table, src_sem, u_sem, table_sem, own_sem,
           in_send, near_recv, in_recv, x_send, x_recv, out_send, out_recv):
    slots = green.shape[2]
    rows = green.shape[4]
    per_group = slots // GROUPS
    per_half = slots // HALVES
    z = lax.axis_index("energy")
    x = lax.axis_index("orb")
    k = lax.axis_index("kpt")
    z_hi, row, core = k // 8, (k // 2) % 4, k % 2

    fetch = pltpu.make_async_copy(lesser, src, src_sem)
    fetch.start()
    fetch_u = pltpu.make_async_copy(coupling, u, u_sem)
    fetch_u.start()
    own = []
    for chunk in range(CHUNKS):
        begin = pl.multiple_of((z + 4 - 2 * core - chunk) % 4 * 128 + k // 2 * rows, rows)
        own.append(
            pltpu.make_async_copy(
                lesser.at[:, pl.ds(begin, rows), :], green.at[chunk, x, 0], own_sem.at[chunk]
            )
        )
        own[-1].start()
    fetch_table = pltpu.make_async_copy(table_in, table, table_sem)
    fetch_table.start()

    def fetched():
        fetch_u.wait()
        fetch_table.wait()

    barrier = pltpu.get_barrier_semaphore()

    def greet(z_to, x_to, k_to):
        pl.semaphore_signal(barrier, inc=1, device_id=(z_to, x_to, k_to), device_id_type=MESH)

    def greet_near(i, carry):
        other = (x * 8 + k % 8 + i) % 32
        greet(z, other // 8, z_hi * 8 + other % 8)
        return carry

    def greet_far(i, carry):
        greet(z, x, (k + 8) // 8 % 2 * 8 + i)
        greet((z + 1) % 4, x, 2 * i)
        greet((z + 2) % 4, x, 2 * i + 1)
        greet((z + 3) % 4, x, 2 * i + 1)
        return carry

    lax.fori_loop(0, 8, greet_far, 0, unroll=True)
    lax.fori_loop(1, 32, greet_near, 0, unroll=True)
    with scope("s_fetch"):
        fetch.wait()
    with scope("s_barrier"):
        pl.semaphore_wait(barrier, 55 + 16 * core)

    def send(source, target, send_sem, recv_sem, place):
        return pltpu.make_async_remote_copy(
            src_ref=source, dst_ref=target, send_sem=send_sem, recv_sem=recv_sem,
            device_id=place, device_id_type=MESH,
        )

    def landed(block, recv_sem):
        send(block, block, x_send, recv_sem, (z, (x + 1) % 4, k)).wait_recv()

    def sent(block, send_sem):
        send(block, block, send_sem, out_recv, (z, (x + 1) % 4, k)).wait_send()

    places = tuple(itertools.product(range(2), NEAR_FIRST, range(2)))

    def deal(chunk, slot, x_step):
        z_step, near, core_step = places[slot]
        z_hi_to, row_to, core_to = (z_hi + z_step) % 2, (row + 4 - near) % 4, (core + core_step) % 2
        tile = (z + 4 - 2 * core_to - chunk) % 4
        begin = pl.multiple_of(tile * 128 + (z_hi_to * 4 + row_to) * rows, rows)
        send(
            src.at[:, pl.ds(begin, rows), :],
            green.at[chunk, x, slot],
            in_send,
            near_recv.at[chunk] if slot < FLIGHT * per_group else in_recv.at[chunk, slot // per_group],
            (z, (x + x_step) % 4, z_hi_to * 8 + row_to * 2 + core_to),
        ).start()

    for chunk, slots_of in DEAL:
        for slot in slots_of:
            for x_step in X_STEPS if slot < FLIGHT * per_group else (0,):
                if (slot, x_step) != (0, 0):
                    deal(chunk, slot, x_step)

    def spread(chunk, group):
        block = green.at[chunk, x, pl.ds(group * per_group, per_group)]
        landed(block, in_recv.at[chunk, group])
        for x_step in X_STEPS[1:]:
            send(block, block, x_send, x_recv.at[chunk, group * 4 // GROUPS], (z, (x + x_step) % 4, k)).start()

    def arrive(chunk, first, last):
        if first == 0:
            own[chunk].wait()
            landed(packed.at[pl.ds(0, 4 * per_group * FLIGHT - 1)], near_recv.at[chunk])
        for quarter in range(first, last):
            spreads = GROUPS // 4 - (FLIGHT if quarter == 0 else 0)
            landed(packed.at[pl.ds(0, 3 * per_group * spreads)], x_recv.at[chunk, quarter])

    def product(chunk, first, last):
        count = slots // 4 * (last - first)
        part = pl.ds(slots // 4 * first, count)

        def at(t, carry):
            lhs = jnp.concatenate(
                [green[chunk, m, part].reshape(count * 2 * rows, 128) for m in range(4)], axis=1
            )
            rhs = jnp.concatenate([u[0, t], u[1, t]], axis=1)
            terms = jnp.dot(lhs, rhs, preferred_element_type=jnp.float32)
            y[chunk, t, part] = terms.reshape(count, 2, rows, 256)
            return carry

        lax.fori_loop(0, 16, at, 0, unroll=True)

    wraps = z == 3 * core

    def target_of(chunk, i):
        far = jnp.where(i % 8 < 4, 2 + i % 8 // 2, 3 - i % 8 // 2)
        z_step = 1 - i // 8
        if chunk:
            z_step = jnp.where(wraps, i // 8, z_step)
        return (z_hi + z_step) % 2 * 8 + (row + far) % 4 * 2 + (core + 1 + i) % 2

    def total(chunk, i):
        target = target_of(chunk, i)
        real = jnp.zeros((rows, 128), jnp.float32)
        imag = jnp.zeros((rows, 128), jnp.float32)
        for slot in range(slots):
            z_step, near, core_step = places[slot]
            point = (z_hi + z_step) % 2 * 8 + (row + near) % 4 * 2 + (core + core_step) % 2
            term = y[chunk, table[target, point], slot]
            real += term[0, :, :128] - term[1, :, 128:]
            imag += term[0, :, 128:] + term[1, :, :128]
        packed[chunk * 16 + i, 0] = real.astype(packed.dtype)
        packed[chunk * 16 + i, 1] = imag.astype(packed.dtype)

    def give(chunk, i):
        tile = (z + 4 - 2 * core - chunk) % 4
        begin = pl.ds(pl.multiple_of(k // 2 * rows, rows), rows)

        def away():
            send(
                packed.at[chunk * 16 + i], out.at[:, z, begin, :], out_send, out_recv,
                (tile, x, target_of(chunk, i)),
            ).start()

        if chunk > 0:
            away()
        else:
            stays = jnp.logical_and(core == 0, i == 15)
            pl.when(jnp.logical_not(stays))(away)

            @pl.when(stays)
            def _():
                out[:, z, begin, :] = packed[15]

    def combine(chunk):
        def at(i, carry):
            total(chunk, i)
            give(chunk, i)
            return carry

        lax.fori_loop(0, 16, at, 0, unroll=True)

    act = {
        "S": spread, "A": arrive, "P": product, "C": combine, "U": fetched,
    }
    for name in ORDER:
        with scope("s_" + name):
            act[name[0]](*(int(digit) for digit in name[1:]))

    with scope("s_drain"):
        sent(u.at[:, pl.ds(0, 3), pl.ds(0, 160 + 64 * FLIGHT), :], in_send)
        sent(u.at[:, pl.ds(0, 4), pl.ds(0, 384 - 48 * FLIGHT), :], x_send)
        for count in (31, 32):

            @pl.when(core == count - 31)
            def _():
                sent(packed.at[pl.ds(0, count)], out_send)
    with scope("s_collect"):
        for count in (31, 32):

            @pl.when(core == count - 31)
            def _():
                landed(packed.at[pl.ds(0, count)], out_recv)


def per_device(lesser, coupling, table):
    rows = 16
    result = pl.pallas_call(
        kernel,
        out_shape=pltpu.VMEM((2, 4, 128, 128), jnp.bfloat16),
        in_specs=[
            pl.BlockSpec(memory_space=pl.ANY),
            pl.BlockSpec(memory_space=pl.ANY),
            pl.BlockSpec(memory_space=pl.ANY),
        ],
        out_specs=pl.BlockSpec(memory_space=pltpu.VMEM),
        scratch_shapes=[
            pltpu.VMEM((2, 512, 128), jnp.bfloat16),
            pltpu.VMEM((CHUNKS, 4, 16, 2, rows, 128), jnp.bfloat16),
            pltpu.VMEM((2, 16, 512, 128), jnp.bfloat16),
            pltpu.VMEM((CHUNKS, 16, 16, 2, rows, 256), jnp.float32),
            pltpu.VMEM((CHUNKS * 16, 2, rows, 128), jnp.bfloat16),
            pltpu.SMEM((16, 16), jnp.int32),
            pltpu.SemaphoreType.DMA,
            pltpu.SemaphoreType.DMA,
            pltpu.SemaphoreType.DMA,
            pltpu.SemaphoreType.DMA((CHUNKS,)),
            pltpu.SemaphoreType.DMA,
            pltpu.SemaphoreType.DMA((CHUNKS,)),
            pltpu.SemaphoreType.DMA((CHUNKS, GROUPS)),
            pltpu.SemaphoreType.DMA,
            pltpu.SemaphoreType.DMA((CHUNKS, 4)),
            pltpu.SemaphoreType.DMA,
            pltpu.SemaphoreType.DMA,
        ],
        compiler_params=pltpu.CompilerParams(collective_id=0, has_side_effects=True),
        name="convolve",
    )(lesser.reshape(2, 512, 128), coupling, table)
    return result.reshape(2, 4, 1, 1, 128, 128)


def solution(mesh):
    return jax.shard_map(
        per_device,
        mesh=mesh,
        in_specs=(P(None, "energy", "kpt", None, None, "orb"), P(None, None, None, "orb"), P()),
        out_specs=P(None, None, "kpt", None, "energy", "orb"),
        check_vma=False,
    )
```

```python
import contextlib
import itertools

import jax
import jax.numpy as jnp
from jax import lax
from jax.experimental import pallas as pl
from jax.experimental.pallas import tpu as pltpu
from jax.sharding import PartitionSpec as P

MESH = pl.DeviceIdType.MESH
scope = contextlib.nullcontext
CHUNKS = 2
GROUPS = 8
HALVES = 2
NEAR_FIRST = (0, 1, 3, 2)
X_STEPS = (0, 2, 1, 3)
FLIGHT = 1
DEAL = ((0, range(16)), (1, range(16)))
ORDER = (
    "S01", "S02", "S03", "S11", "S12", "S04", "S13", "S05", "S06", "S07", "A002", "U", "P002", "S14",
    "S15", "S16", "S17", "A102", "P102", "A023", "P023", "A034", "P034", "C0", "A123", "P123", "A134",
    "P134", "C1",
)


def kernel(lesser, coupling, table_in, out, src, green, u, y, packed, table, src_sem, u_sem, table_sem, own_sem,
           in_send, near_recv, in_recv, x_send, x_recv, out_send, out_recv):
    slots = green.shape[2]
    rows = green.shape[4]
    per_group = slots // GROUPS
    per_half = slots // HALVES
    z = lax.axis_index("energy")
    x = lax.axis_index("orb")
    k = lax.axis_index("kpt")
    z_hi, row, core = k // 8, (k // 2) % 4, k % 2

    fetch = pltpu.make_async_copy(lesser, src, src_sem)
    fetch.start()
    fetch_u = pltpu.make_async_copy(coupling, u, u_sem)
    fetch_u.start()
    own = []
    for chunk in range(CHUNKS):
        begin = pl.multiple_of((z + 4 - 2 * core - chunk) % 4 * 128 + k // 2 * rows, rows)
        own.append(
            pltpu.make_async_copy(
                lesser.at[:, pl.ds(begin, rows), :], green.at[chunk, x, 0], own_sem.at[chunk]
            )
        )
        own[-1].start()
    fetch_table = pltpu.make_async_copy(table_in, table, table_sem)
    fetch_table.start()

    def fetched():
        fetch_u.wait()
        fetch_table.wait()

    barrier = pltpu.get_barrier_semaphore()

    def greet(z_to, x_to, k_to):
        pl.semaphore_signal(barrier, inc=1, device_id=(z_to, x_to, k_to), device_id_type=MESH)

    def greet_near(i, carry):
        other = (x * 8 + k % 8 + i) % 32
        greet(z, other // 8, z_hi * 8 + other % 8)
        return carry

    def greet_far(i, carry):
        greet(z, x, (k + 8) // 8 % 2 * 8 + i)
        greet((z + 1) % 4, x, 2 * i)
        greet((z + 2) % 4, x, 2 * i + 1)
        greet((z + 3) % 4, x, 2 * i + 1)
        return carry

    lax.fori_loop(0, 8, greet_far, 0, unroll=True)
    lax.fori_loop(1, 32, greet_near, 0, unroll=True)
    with scope("s_fetch"):
        fetch.wait()
    with scope("s_barrier"):
        pl.semaphore_wait(barrier, 55 + 16 * core)

    def send(source, target, send_sem, recv_sem, place):
        return pltpu.make_async_remote_copy(
            src_ref=source, dst_ref=target, send_sem=send_sem, recv_sem=recv_sem,
            device_id=place, device_id_type=MESH,
        )

    def landed(block, recv_sem):
        send(block, block, x_send, recv_sem, (z, (x + 1) % 4, k)).wait_recv()

    def sent(block, send_sem):
        send(block, block, send_sem, out_recv, (z, (x + 1) % 4, k)).wait_send()

    places = tuple(itertools.product(range(2), NEAR_FIRST, range(2)))

    def deal(chunk, slot, x_step):
        z_step, near, core_step = places[slot]
        z_hi_to, row_to, core_to = (z_hi + z_step) % 2, (row + 4 - near) % 4, (core + core_step) % 2
        tile = (z + 4 - 2 * core_to - chunk) % 4
        begin = pl.multiple_of(tile * 128 + (z_hi_to * 4 + row_to) * rows, rows)
        send(
            src.at[:, pl.ds(begin, rows), :],
            green.at[chunk, x, slot],
            in_send,
            near_recv.at[chunk] if slot < FLIGHT * per_group else in_recv.at[chunk, slot // per_group],
            (z, (x + x_step) % 4, z_hi_to * 8 + row_to * 2 + core_to),
        ).start()

    for chunk, slots_of in DEAL:
        for slot in slots_of:
            for x_step in X_STEPS if slot < FLIGHT * per_group else (0,):
                if (slot, x_step) != (0, 0):
                    deal(chunk, slot, x_step)

    def spread(chunk, group):
        block = green.at[chunk, x, pl.ds(group * per_group, per_group)]
        landed(block, in_recv.at[chunk, group])
        for x_step in X_STEPS[1:]:
            send(block, block, x_send, x_recv.at[chunk, group * 4 // GROUPS], (z, (x + x_step + 2 * core * (x_step % 2)) % 4, k)).start()

    def arrive(chunk, first, last):
        if first == 0:
            own[chunk].wait()
            landed(packed.at[pl.ds(0, 4 * per_group * FLIGHT - 1)], near_recv.at[chunk])
        for quarter in range(first, last):
            spreads = GROUPS // 4 - (FLIGHT if quarter == 0 else 0)
            landed(packed.at[pl.ds(0, 3 * per_group * spreads)], x_recv.at[chunk, quarter])

    def product(chunk, first, last):
        count = slots // 4 * (last - first)
        part = pl.ds(slots // 4 * first, count)

        def at(t, carry):
            lhs = jnp.concatenate(
                [green[chunk, m, part].reshape(count * 2 * rows, 128) for m in range(4)], axis=1
            )
            rhs = jnp.concatenate([u[0, t], u[1, t]], axis=1)
            terms = jnp.dot(lhs, rhs, preferred_element_type=jnp.float32)
            y[chunk, t, part] = terms.reshape(count, 2, rows, 256)
            return carry

        lax.fori_loop(0, 16, at, 0, unroll=True)

    wraps = z == 3 * core

    def target_of(chunk, i):
        far = jnp.where(i % 8 < 4, 2 + i % 8 // 2, 3 - i % 8 // 2)
        z_step = 1 - i // 8
        if chunk:
            z_step = jnp.where(wraps, i // 8, z_step)
        return (z_hi + z_step) % 2 * 8 + (row + far) % 4 * 2 + (core + 1 + i) % 2

    def total(chunk, i):
        target = target_of(chunk, i)
        real = jnp.zeros((rows, 128), jnp.float32)
        imag = jnp.zeros((rows, 128), jnp.float32)
        for slot in range(slots):
            z_step, near, core_step = places[slot]
            point = (z_hi + z_step) % 2 * 8 + (row + near) % 4 * 2 + (core + core_step) % 2
            term = y[chunk, table[target, point], slot]
            real += term[0, :, :128] - term[1, :, 128:]
            imag += term[0, :, 128:] + term[1, :, :128]
        packed[chunk * 16 + i, 0] = real.astype(packed.dtype)
        packed[chunk * 16 + i, 1] = imag.astype(packed.dtype)

    def give(chunk, i):
        tile = (z + 4 - 2 * core - chunk) % 4
        begin = pl.ds(pl.multiple_of(k // 2 * rows, rows), rows)

        def away():
            send(
                packed.at[chunk * 16 + i], out.at[:, z, begin, :], out_send, out_recv,
                (tile, x, target_of(chunk, i)),
            ).start()

        if chunk > 0:
            away()
        else:
            stays = jnp.logical_and(core == 0, i == 15)
            pl.when(jnp.logical_not(stays))(away)

            @pl.when(stays)
            def _():
                out[:, z, begin, :] = packed[15]

    def combine(chunk):
        def at(i, carry):
            total(chunk, i)
            give(chunk, i)
            return carry

        lax.fori_loop(0, 16, at, 0, unroll=True)

    act = {
        "S": spread, "A": arrive, "P": product, "C": combine, "U": fetched,
    }
    for name in ORDER:
        with scope("s_" + name):
            act[name[0]](*(int(digit) for digit in name[1:]))

    with scope("s_drain"):
        sent(u.at[:, pl.ds(0, 3), pl.ds(0, 160 + 64 * FLIGHT), :], in_send)
        sent(u.at[:, pl.ds(0, 4), pl.ds(0, 384 - 48 * FLIGHT), :], x_send)
        for count in (31, 32):

            @pl.when(core == count - 31)
            def _():
                sent(packed.at[pl.ds(0, count)], out_send)
    with scope("s_collect"):
        for count in (31, 32):

            @pl.when(core == count - 31)
            def _():
                landed(packed.at[pl.ds(0, count)], out_recv)


def per_device(lesser, coupling, table):
    rows = 16
    result = pl.pallas_call(
        kernel,
        out_shape=pltpu.VMEM((2, 4, 128, 128), jnp.bfloat16),
        in_specs=[
            pl.BlockSpec(memory_space=pl.ANY),
            pl.BlockSpec(memory_space=pl.ANY),
            pl.BlockSpec(memory_space=pl.ANY),
        ],
        out_specs=pl.BlockSpec(memory_space=pltpu.VMEM),
        scratch_shapes=[
            pltpu.VMEM((2, 512, 128), jnp.bfloat16),
            pltpu.VMEM((CHUNKS, 4, 16, 2, rows, 128), jnp.bfloat16),
            pltpu.VMEM((2, 16, 512, 128), jnp.bfloat16),
            pltpu.VMEM((CHUNKS, 16, 16, 2, rows, 256), jnp.float32),
            pltpu.VMEM((CHUNKS * 16, 2, rows, 128), jnp.bfloat16),
            pltpu.SMEM((16, 16), jnp.int32),
            pltpu.SemaphoreType.DMA,
            pltpu.SemaphoreType.DMA,
            pltpu.SemaphoreType.DMA,
            pltpu.SemaphoreType.DMA((CHUNKS,)),
            pltpu.SemaphoreType.DMA,
            pltpu.SemaphoreType.DMA((CHUNKS,)),
            pltpu.SemaphoreType.DMA((CHUNKS, GROUPS)),
            pltpu.SemaphoreType.DMA,
            pltpu.SemaphoreType.DMA((CHUNKS, 4)),
            pltpu.SemaphoreType.DMA,
            pltpu.SemaphoreType.DMA,
        ],
        compiler_params=pltpu.CompilerParams(collective_id=0, has_side_effects=True),
        name="convolve",
    )(lesser.reshape(2, 512, 128), coupling, table)
    return result.reshape(2, 4, 1, 1, 128, 128)


def solution(mesh):
    return jax.shard_map(
        per_device,
        mesh=mesh,
        in_specs=(P(None, "energy", "kpt", None, None, "orb"), P(None, None, None, "orb"), P()),
        out_specs=P(None, None, "kpt", None, "energy", "orb"),
        check_vma=False,
    )
```

```python
import contextlib
import itertools

import jax
import jax.numpy as jnp
from jax import lax
from jax.experimental import pallas as pl
from jax.experimental.pallas import tpu as pltpu
from jax.sharding import PartitionSpec as P

MESH = pl.DeviceIdType.MESH
scope = contextlib.nullcontext
CHUNKS = 2
GROUPS = 8
HALVES = 2
NEAR_FIRST = (0, 1, 3, 2)
X_STEPS = (0, 2, 1, 3)
FLIGHT = 1
DEAL = ((0, range(8, 16)), (0, range(8)), (1, range(16)))
ORDER = (
    "S01", "S02", "S03", "S11", "S12", "S04", "S13", "S05", "S06", "S07", "A002", "U", "P002", "S14",
    "S15", "S16", "S17", "A102", "P102", "A023", "P023", "A034", "P034", "C0", "A123", "P123", "A134",
    "P134", "C1",
)


def kernel(lesser, coupling, table_in, out, src, green, u, y, packed, table, src_sem, u_sem, table_sem, own_sem,
           in_send, near_recv, in_recv, x_send, x_recv, out_send, out_recv):
    slots = green.shape[2]
    rows = green.shape[4]
    per_group = slots // GROUPS
    per_half = slots // HALVES
    z = lax.axis_index("energy")
    x = lax.axis_index("orb")
    k = lax.axis_index("kpt")
    z_hi, row, core = k // 8, (k // 2) % 4, k % 2

    fetch = pltpu.make_async_copy(lesser, src, src_sem)
    fetch.start()
    fetch_u = pltpu.make_async_copy(coupling, u, u_sem)
    fetch_u.start()
    own = []
    for chunk in range(CHUNKS):
        begin = pl.multiple_of((z + 4 - 2 * core - chunk) % 4 * 128 + k // 2 * rows, rows)
        own.append(
            pltpu.make_async_copy(
                lesser.at[:, pl.ds(begin, rows), :], green.at[chunk, x, 0], own_sem.at[chunk]
            )
        )
        own[-1].start()
    fetch_table = pltpu.make_async_copy(table_in, table, table_sem)
    fetch_table.start()

    def fetched():
        fetch_u.wait()
        fetch_table.wait()

    barrier = pltpu.get_barrier_semaphore()

    def greet(z_to, x_to, k_to):
        pl.semaphore_signal(barrier, inc=1, device_id=(z_to, x_to, k_to), device_id_type=MESH)

    def greet_near(i, carry):
        other = (x * 8 + k % 8 + i) % 32
        greet(z, other // 8, z_hi * 8 + other % 8)
        return carry

    def greet_far(i, carry):
        greet(z, x, (k + 8) // 8 % 2 * 8 + i)
        greet((z + 1) % 4, x, 2 * i)
        greet((z + 2) % 4, x, 2 * i + 1)
        greet((z + 3) % 4, x, 2 * i + 1)
        return carry

    lax.fori_loop(0, 8, greet_far, 0, unroll=True)
    lax.fori_loop(1, 32, greet_near, 0, unroll=True)
    with scope("s_fetch"):
        fetch.wait()
    with scope("s_barrier"):
        pl.semaphore_wait(barrier, 55 + 16 * core)

    def send(source, target, send_sem, recv_sem, place):
        return pltpu.make_async_remote_copy(
            src_ref=source, dst_ref=target, send_sem=send_sem, recv_sem=recv_sem,
            device_id=place, device_id_type=MESH,
        )

    def landed(block, recv_sem):
        send(block, block, x_send, recv_sem, (z, (x + 1) % 4, k)).wait_recv()

    def sent(block, send_sem):
        send(block, block, send_sem, out_recv, (z, (x + 1) % 4, k)).wait_send()

    places = tuple(itertools.product(range(2), NEAR_FIRST, range(2)))

    def deal(chunk, slot, x_step):
        z_step, near, core_step = places[slot]
        z_hi_to, row_to, core_to = (z_hi + z_step) % 2, (row + 4 - near) % 4, (core + core_step) % 2
        tile = (z + 4 - 2 * core_to - chunk) % 4
        begin = pl.multiple_of(tile * 128 + (z_hi_to * 4 + row_to) * rows, rows)
        send(
            src.at[:, pl.ds(begin, rows), :],
            green.at[chunk, x, slot],
            in_send,
            near_recv.at[chunk] if slot < FLIGHT * per_group else in_recv.at[chunk, slot // per_group],
            (z, (x + x_step) % 4, z_hi_to * 8 + row_to * 2 + core_to),
        ).start()

    for chunk, slots_of in DEAL:
        for slot in slots_of:
            for x_step in X_STEPS if slot < FLIGHT * per_group else (0,):
                if (slot, x_step) != (0, 0):
                    deal(chunk, slot, x_step)

    def spread(chunk, group):
        block = green.at[chunk, x, pl.ds(group * per_group, per_group)]
        landed(block, in_recv.at[chunk, group])
        for x_step in X_STEPS[1:]:
            send(block, block, x_send, x_recv.at[chunk, group * 4 // GROUPS], (z, (x + x_step) % 4, k)).start()

    def arrive(chunk, first, last):
        if first == 0:
            own[chunk].wait()
            landed(packed.at[pl.ds(0, 4 * per_group * FLIGHT - 1)], near_recv.at[chunk])
        for quarter in range(first, last):
            spreads = GROUPS // 4 - (FLIGHT if quarter == 0 else 0)
            landed(packed.at[pl.ds(0, 3 * per_group * spreads)], x_recv.at[chunk, quarter])

    def product(chunk, first, last):
        count = slots // 4 * (last - first)
        part = pl.ds(slots // 4 * first, count)

        def at(t, carry):
            lhs = jnp.concatenate(
                [green[chunk, m, part].reshape(count * 2 * rows, 128) for m in range(4)], axis=1
            )
            rhs = jnp.concatenate([u[0, t], u[1, t]], axis=1)
            terms = jnp.dot(lhs, rhs, preferred_element_type=jnp.float32)
            y[chunk, t, part] = terms.reshape(count, 2, rows, 256)
            return carry

        lax.fori_loop(0, 16, at, 0, unroll=True)

    wraps = z == 3 * core

    def target_of(chunk, i):
        far = jnp.where(i % 8 < 4, 2 + i % 8 // 2, 3 - i % 8 // 2)
        z_step = 1 - i // 8
        if chunk:
            z_step = jnp.where(wraps, i // 8, z_step)
        return (z_hi + z_step) % 2 * 8 + (row + far) % 4 * 2 + (core + 1 + i) % 2

    def total(chunk, i):
        target = target_of(chunk, i)
        real = jnp.zeros((rows, 128), jnp.float32)
        imag = jnp.zeros((rows, 128), jnp.float32)
        for slot in range(slots):
            z_step, near, core_step = places[slot]
            point = (z_hi + z_step) % 2 * 8 + (row + near) % 4 * 2 + (core + core_step) % 2
            term = y[chunk, table[target, point], slot]
            real += term[0, :, :128] - term[1, :, 128:]
            imag += term[0, :, 128:] + term[1, :, :128]
        packed[chunk * 16 + i, 0] = real.astype(packed.dtype)
        packed[chunk * 16 + i, 1] = imag.astype(packed.dtype)

    def give(chunk, i):
        tile = (z + 4 - 2 * core - chunk) % 4
        begin = pl.ds(pl.multiple_of(k // 2 * rows, rows), rows)

        def away():
            send(
                packed.at[chunk * 16 + i], out.at[:, z, begin, :], out_send, out_recv,
                (tile, x, target_of(chunk, i)),
            ).start()

        if chunk > 0:
            away()
        else:
            stays = jnp.logical_and(core == 0, i == 15)
            pl.when(jnp.logical_not(stays))(away)

            @pl.when(stays)
            def _():
                out[:, z, begin, :] = packed[15]

    def combine(chunk):
        def at(i, carry):
            total(chunk, i)
            give(chunk, i)
            return carry

        lax.fori_loop(0, 16, at, 0, unroll=True)

    act = {
        "S": spread, "A": arrive, "P": product, "C": combine, "U": fetched,
    }
    for name in ORDER:
        with scope("s_" + name):
            act[name[0]](*(int(digit) for digit in name[1:]))

    with scope("s_drain"):
        sent(u.at[:, pl.ds(0, 3), pl.ds(0, 160 + 64 * FLIGHT), :], in_send)
        sent(u.at[:, pl.ds(0, 4), pl.ds(0, 384 - 48 * FLIGHT), :], x_send)
        for count in (31, 32):

            @pl.when(core == count - 31)
            def _():
                sent(packed.at[pl.ds(0, count)], out_send)
    with scope("s_collect"):
        for count in (31, 32):

            @pl.when(core == count - 31)
            def _():
                landed(packed.at[pl.ds(0, count)], out_recv)


def per_device(lesser, coupling, table):
    rows = 16
    result = pl.pallas_call(
        kernel,
        out_shape=pltpu.VMEM((2, 4, 128, 128), jnp.bfloat16),
        in_specs=[
            pl.BlockSpec(memory_space=pl.ANY),
            pl.BlockSpec(memory_space=pl.ANY),
            pl.BlockSpec(memory_space=pl.ANY),
        ],
        out_specs=pl.BlockSpec(memory_space=pltpu.VMEM),
        scratch_shapes=[
            pltpu.VMEM((2, 512, 128), jnp.bfloat16),
            pltpu.VMEM((CHUNKS, 4, 16, 2, rows, 128), jnp.bfloat16),
            pltpu.VMEM((2, 16, 512, 128), jnp.bfloat16),
            pltpu.VMEM((CHUNKS, 16, 16, 2, rows, 256), jnp.float32),
            pltpu.VMEM((CHUNKS * 16, 2, rows, 128), jnp.bfloat16),
            pltpu.SMEM((16, 16), jnp.int32),
            pltpu.SemaphoreType.DMA,
            pltpu.SemaphoreType.DMA,
            pltpu.SemaphoreType.DMA,
            pltpu.SemaphoreType.DMA((CHUNKS,)),
            pltpu.SemaphoreType.DMA,
            pltpu.SemaphoreType.DMA((CHUNKS,)),
            pltpu.SemaphoreType.DMA((CHUNKS, GROUPS)),
            pltpu.SemaphoreType.DMA,
            pltpu.SemaphoreType.DMA((CHUNKS, 4)),
            pltpu.SemaphoreType.DMA,
            pltpu.SemaphoreType.DMA,
        ],
        compiler_params=pltpu.CompilerParams(collective_id=0, has_side_effects=True),
        name="convolve",
    )(lesser.reshape(2, 512, 128), coupling, table)
    return result.reshape(2, 4, 1, 1, 128, 128)


def solution(mesh):
    return jax.shard_map(
        per_device,
        mesh=mesh,
        in_specs=(P(None, "energy", "kpt", None, None, "orb"), P(None, None, None, "orb"), P()),
        out_specs=P(None, None, "kpt", None, "energy", "orb"),
        check_vma=False,
    )
```
